32 devices in a mesh: blk: 4 (over z), tp: 8 (over y, x, core).
Axes of the slice: x: 2, y: 2, z: 4, core: 2. Of those that a mesh axis runs over, the one named last changes fastest.
Arguments:
- input_pool: bfloat16 [4096, 1792], P(None, 'tp'), may hold values from -6 to 6
- teacher_pool: bfloat16 [4096, 1792], P(None, 'tp'), may hold values from -6 to 6
- gate_weight: bfloat16 [1792, 9472], P(None, 'tp'), may hold values from -0.125 to 0.125
- up_weight: bfloat16 [1792, 9472], P(None, 'tp'), may hold values from -0.125 to 0.125
- params: float32 [4, 9472, 1792], P('blk', 'tp'), may hold values from -6 to 6
- batch_ids: int32 [4, 1024], replicated, may hold values from 0 to 4095
- cycle_order: int32 [4], replicated, may hold values from 0 to 3, each once
- edge_weight: float32 [4], replicated, may hold values from 0.1 to 0.45
Outputs:
- updated: float32 [4, 9472, 1792], P('blk', 'tp')
The draws below stay inside these ranges and needn't reach their ends.
Inputs may be any that keep to these rules, and one draw needn't show every extreme that they name: `cycle_order`: the 4 cycle positions name 4 different agents.
All inputs are finite; a program needn't handle non-finite values.
Results may differ from the reference program's by a relative error of at most 0.0061.
Values may be sent and summed in bfloat16 or wider, within the bound.
A program may use at most 128 MiB of HBM per device.

```python
import math
import jax
import jax.numpy as jnp
from jax import lax

D = 1792
FF = 9472
TOK = 1024
POOL = 4096
AGENTS = 4


def set_ends(entries, key, least, top_value):
    index_at = [jax.random.randint(jax.random.fold_in(key, axis), (), 0, length) for axis, length in enumerate(entries.shape)]
    widest = entries.shape.index(max(entries.shape))
    next_to = index_at[:widest] + [(index_at[widest] + 1) % entries.shape[widest]] + index_at[widest + 1:]
    return entries.at[tuple(index_at)].set(least).at[tuple(next_to)].set(top_value)


def block_scale(stream_key, shape, cuts, smallest, largest):
    def one(axis_at, shards_of):
        draws = jax.random.uniform(jax.random.fold_in(jax.random.fold_in(stream_key, 6), axis_at), (shards_of,), jnp.float32, smallest / len(cuts), largest / len(cuts))
        return jnp.repeat(jnp.exp(draws), shape[axis_at] // shards_of).reshape((-1,) + (1,) * (len(shape) - axis_at - 1))

    loudness = one(*cuts[0])
    for cut in cuts[1:]:
        loudness = loudness * one(*cut)
    return loudness


def scatter_about(stream_key, shape, width, limit, split=(), dtype=jnp.bfloat16):
    result = jax.random.normal(stream_key, shape, jnp.float32) * width
    if len(split) > 0:
        result = block_scale(stream_key, shape, split, -0.22, 0.18) * result
    return jnp.clip(result, min=-limit, max=limit).astype(dtype)


def setup_inputs(seed: int = 0) -> dict:
    splits = jax.random.split(jax.random.key(seed), 9)
    input_pool = scatter_about(splits[0], (POOL, D), 1.0, 6.0, ((1, 8),))
    teacher_pool = scatter_about(splits[1], (POOL, D), 1.0, 6.0, ((1, 8),))
    gate_weight = scatter_about(splits[2], (D, FF), D ** -0.5, 0.125, ((1, 8),))
    up_weight = scatter_about(splits[3], (D, FF), D ** -0.5, 0.125, ((1, 8),))
    params = scatter_about(splits[4], (AGENTS, FF, D), 1.0, 6.0, ((0, 4), (1, 8)), jnp.float32)
    batch_ids = set_ends(jax.random.randint(splits[5], (AGENTS, TOK), 0, POOL), jax.random.fold_in(splits[5], 1), 0, POOL - 1).astype(jnp.int32)
    cycle_order = jax.random.permutation(splits[6], AGENTS).astype(jnp.int32)
    edge_weight = jnp.clip(jnp.exp(jax.random.uniform(splits[7], (AGENTS,), jnp.float32, math.log(0.1), math.log(0.45))), 0.1, 0.45)
    return {"input_pool": input_pool, "teacher_pool": teacher_pool, "gate_weight": gate_weight, "up_weight": up_weight, "params": params, "batch_ids": batch_ids, "cycle_order": cycle_order, "edge_weight": edge_weight}


def reference(input_pool, teacher_pool, gate_weight, up_weight, params, batch_ids, cycle_order, edge_weight):
    scale = float(FF) ** (-0.5)
    step_rate = 2.0
    batches = batch_ids[cycle_order]

    def make_hidden(batch):
        rows = input_pool[batch]
        gate = jnp.dot(rows, gate_weight, preferred_element_type=jnp.float32)
        up = jnp.dot(rows, up_weight, preferred_element_type=jnp.float32)
        return (jax.nn.silu(gate) * up).astype(jnp.bfloat16)
    hidden = lax.map(make_hidden, batches)
    targets = teacher_pool[batches]

    def one_grad(items):
        hid, tgt, weights = items
        out = scale * jnp.dot(hid, weights.astype(jnp.bfloat16), preferred_element_type=jnp.float32)
        resid = (out - tgt.astype(jnp.float32)).astype(jnp.bfloat16)
        return scale * jnp.dot(hid.T, resid, preferred_element_type=jnp.float32)

    def gradient(field):
        return lax.map(one_grad, (hidden, targets, field))
    weight_next = edge_weight[:, None, None]
    weight_prev = jnp.roll(edge_weight, 1)[:, None, None]
    weight_self = 1.0 - weight_next - weight_prev

    def mix(field):
        return weight_self * field + weight_next * jnp.roll(field, -1, 0) + weight_prev * jnp.roll(field, 1, 0)
    grad_first = gradient(params)
    moved = mix(params) - step_rate * grad_first
    grad_second = gradient(moved)
    tracker = mix(grad_first) + grad_second - grad_first
    return mix(moved) - step_rate * tracker
```

```python
import jax
import jax.numpy as jnp
from jax import lax
from jax.sharding import PartitionSpec as P


def shifted(array, axis, by):
    count = lax.axis_size(axis)
    return lax.ppermute(array, axis, [(i, (i + by) % count) for i in range(count)])


def body(
    input_pool, teacher_pool, gate_weight, up_weight, params, batch_ids, cycle_order, edge_weight
):
    step_rate = 2.0
    groups = lax.axis_size("tp")
    place = lax.axis_index("blk")
    agents = cycle_order.shape[0]
    slots = jnp.arange(agents, dtype=jnp.int32)
    here = slots == place
    before = slots == (place + agents - 1) % agents
    agent = jnp.sum(jnp.where(here, cycle_order, 0))
    weight_next = jnp.sum(jnp.where(here, edge_weight, 0.0))
    weight_prev = jnp.sum(jnp.where(before, edge_weight, 0.0))
    weight_self = 1.0 - weight_next - weight_prev
    batch = lax.dynamic_slice_in_dim(batch_ids, agent, 1, 0)[0]
    field_rows = params.shape[1]
    cut = field_rows // 2
    spans = ((0, cut), (cut, field_rows))

    def exchanged(half):
        lower = shifted(half, "blk", 1)
        upper = shifted(half, "blk", -1)
        return lower, upper

    def mixed(own, pair):
        lower, upper = pair
        return (
            weight_self * own
            + weight_next * upper.astype(jnp.float32)
            + weight_prev * lower.astype(jnp.float32)
        )

    start = [params[0, lo:hi] for lo, hi in spans]
    start_half = [part.astype(jnp.bfloat16) for part in start]
    batch, *start_half = lax.optimization_barrier((batch, *start_half))
    near_early = exchanged(start_half[0])

    inputs_local = jnp.take(input_pool, batch, axis=0)
    hidden_dev = gate_weight.shape[1]
    scale = float(hidden_dev * groups) ** (-0.5)
    rows = lax.all_gather(inputs_local, "tp", axis=1, tiled=True)
    gate = jnp.dot(rows, gate_weight, preferred_element_type=jnp.float32)
    up = jnp.dot(rows, up_weight, preferred_element_type=jnp.float32)
    hidden = (jax.nn.silu(gate) * up).astype(jnp.bfloat16)
    teacher_local = jnp.take(teacher_pool, batch, axis=0)
    own_width = teacher_local.shape[1]
    target_part = lax.dynamic_update_slice(
        jnp.zeros((teacher_local.shape[0], own_width * groups), teacher_local.dtype),
        teacher_local,
        (0, lax.axis_index("tp") * own_width),
    )

    def share(parts):
        weights_half = jnp.concatenate(parts, axis=0)
        partial_out = scale * jnp.dot(hidden, weights_half, preferred_element_type=jnp.float32)
        return (partial_out - target_part.astype(jnp.float32)).astype(jnp.bfloat16)

    def gradient(resid, lo, hi):
        return scale * lax.dot_general(
            hidden[:, lo:hi], resid, (((0,), (0,)), ((), ())), preferred_element_type=jnp.float32
        )

    share_first = share(start_half)
    share_first, half_late = lax.optimization_barrier((share_first, start_half[1]))
    resid_first = lax.psum(share_first, "tp")
    start_near = (near_early, exchanged(half_late))
    moved_half, bases, combined_near = [], [], []
    for k, ((lo, hi), own, near) in enumerate(zip(spans, start, start_near)):
        if k:
            near, _ = lax.optimization_barrier((near, (moved_half[-1], joint_half, bases[-1])))
        grad = gradient(resid_first, lo, hi)
        blend = mixed(own, near)
        joint = blend - 2.0 * step_rate * grad
        moved_half.append((blend - step_rate * grad).astype(jnp.bfloat16))
        bases.append(weight_self * joint + step_rate * grad)
        joint_half = joint.astype(jnp.bfloat16)
        combined_near.append(exchanged(joint_half))
    share_second = share(moved_half)
    resid_second = lax.psum(share_second, "tp")
    result = []
    for (lo, hi), base, (lower, upper) in zip(spans, bases, combined_near):
        base = base - step_rate * gradient(resid_second, lo, hi)
        result.append(
            base
            + weight_next * upper.astype(jnp.float32)
            + weight_prev * lower.astype(jnp.float32)
        )
    return jnp.concatenate(result, axis=0)[None]


def solution(mesh):
    placed = (
        P(None, "tp"),
        P(None, "tp"),
        P(None, "tp"),
        P(None, "tp"),
        P("blk", "tp", None),
        P(),
        P(),
        P(),
    )

    return jax.shard_map(
        body, mesh=mesh, in_specs=placed, out_specs=P("blk", "tp", None), check_vma=False
    )
```
